32 devices in a mesh: date: 16 (over z, y, x), pix: 2 (over core).
Axes of the slice: x: 2, y: 2, z: 4, core: 2. Of those that a mesh axis runs over, the one named last changes fastest.
Arguments:
- reflect: bfloat16 [64, 6, 16384], P('date', None, 'pix'), may hold values from -8 to 8
- cloud_free: int32 [64, 16384], P('date', 'pix'), may hold values from 0 to 1, as said below
- days: int32 [64], P('date'), may hold values from 1 to 2079, as said below
Outputs:
- median: float32 [6, 16384], P(None, 'pix')
- slope: float32 [6, 16384], P(None, 'pix')
The draws below stay inside these ranges and needn't reach their ends.
Inputs may be any that keep to these rules, and one draw needn't show every extreme that they name: `cloud_free`: every pixel is clear on at least one of the first 32 dates and on at least one of the others; clear shares differ between tiles. `days`: strictly increasing.
All inputs are finite; a program needn't handle non-finite values.
Results may differ from the reference program's by a relative error of at most 0.0003.
Values may be sent and summed in bfloat16 or wider, within the bound.
A program may use at most 64 MiB of HBM per device.

```python
import jax
import jax.numpy as jnp
from jax import lax

DATES = 64
BANDS = 6
PIX_DEV = 8192
PIXELS = 16384


def draw_reflect(key, part):
    keys = jax.random.split(key, 4)
    tiles = PIXELS // PIX_DEV
    region = jax.random.normal(keys[0], (1, BANDS, tiles), jnp.float32)
    haze = 0.6 * jax.random.normal(keys[1], (DATES, BANDS, 1), jnp.float32)
    tile_date = 0.5 * jax.random.normal(keys[2], (DATES, BANDS, tiles), jnp.float32)
    base = jnp.repeat(region + tile_date, PIX_DEV, axis=2) + haze
    noise = 0.8 * jax.random.normal(keys[3], (DATES, BANDS, PIXELS), jnp.float32)
    return jnp.clip(base + noise, -8.0, 8.0).astype(jnp.bfloat16)


def draw_cloud_free(key, part):
    keys = jax.random.split(key, 4)
    tiles = PIXELS // PIX_DEV
    cloudy = jnp.repeat(jax.random.randint(keys[0], (tiles,), 10, 85), PIX_DEV)
    rolls = jax.random.randint(keys[1], (DATES, PIXELS), 0, 100)
    clear = rolls >= cloudy[None, :]
    first = jax.random.randint(keys[2], (PIXELS,), 0, DATES // 2)
    second = jax.random.randint(keys[3], (PIXELS,), DATES // 2, DATES)
    rows = jnp.arange(DATES, dtype=jnp.int32)[:, None]
    clear = clear | (rows == first[None, :]) | (rows == second[None, :])
    return clear.astype(jnp.int32)


def draw_days(key, part):
    keys = jax.random.split(key, 2)
    start = jax.random.randint(keys[0], (), 0, 31)
    gaps = jax.random.randint(keys[1], (DATES,), 1, 33)
    raw = (start + jnp.cumsum(gaps)).astype(jnp.int32)
    index = jnp.arange(DATES, dtype=jnp.int32)
    raw = jnp.where(index == 0, jnp.int32(1), raw)
    raw = jnp.where(index == DATES - 1, jnp.int32(31 + 32 * DATES), raw)
    return raw.astype(jnp.int32)


def setup_inputs(seed: int = 0) -> dict:
    arg_keys = jax.random.split(jax.random.key(seed), 4)
    reflect = draw_reflect(jax.random.fold_in(arg_keys[3], 71), 0)
    cloud_free = draw_cloud_free(jax.random.fold_in(arg_keys[3], 71), 0)
    days = draw_days(jax.random.fold_in(arg_keys[3], 71), 0)
    return {"reflect": reflect, "cloud_free": cloud_free, "days": days}


ridge = 1.0


def rank_block(pair):
    xb, mb = pair
    zeros = jnp.zeros(xb.shape, jnp.float32)

    def step(i, carry):
        less, equal = carry
        xt = lax.dynamic_index_in_dim(xb, i, 0, keepdims=True)
        mt = lax.dynamic_index_in_dim(mb, i, 0, keepdims=True)[:, None, :]
        less = less + mt * (xt < xb).astype(jnp.float32)
        equal = equal + mt * (xt == xb).astype(jnp.float32)
        return (less, equal)

    less, equal = lax.fori_loop(0, xb.shape[0], step, (zeros, zeros))
    count = jnp.sum(mb, 0)
    lower = jnp.floor((count - 1.0) / 2.0)
    upper = jnp.floor(count / 2.0)

    def pick(level):
        chosen = mb[:, None, :] * ((less <= level) & (level < less + equal)).astype(jnp.float32)
        return jnp.sum(chosen * xb, 0) / jnp.maximum(jnp.sum(chosen, 0), 1.0)

    return 0.5 * (pick(lower) + pick(upper))


def reference(reflect, cloud_free, days):
    x = reflect.astype(jnp.float32)
    m = cloud_free.astype(jnp.float32)
    t = days.astype(jnp.float32) / 365.0
    csum = jnp.sum(x * m[:, None, :], 2)
    cnt = jnp.sum(m, 1)
    scene_mean = csum / jnp.maximum(cnt, 1.0)[:, None]
    y = x - scene_mean[:, :, None]
    s0 = jnp.sum(m, 0)
    s1 = jnp.sum(t[:, None] * m, 0)
    s2 = jnp.sum((t * t)[:, None] * m, 0)
    sy = jnp.sum(m[:, None, :] * y, 0)
    sty = jnp.sum((t[:, None] * m)[:, None, :] * y, 0)
    first = s0 + ridge
    det = first * (s2 + ridge) - s1 * s1
    slope = (first[None, :] * sty - s1[None, :] * sy) / det[None, :]
    blocks = PIXELS // PIX_DEV
    xs = x.reshape(DATES, BANDS, blocks, PIX_DEV).transpose(2, 0, 1, 3)
    ms = m.reshape(DATES, blocks, PIX_DEV).transpose(1, 0, 2)
    med = lax.map(rank_block, (xs, ms))
    median = med.transpose(1, 0, 2).reshape(BANDS, PIXELS)
    return median, slope
```

```python
import functools

import jax
import jax.numpy as jnp
from jax import lax
from jax.experimental import pallas as pl
from jax.experimental.pallas import tpu as pltpu
from jax.sharding import PartitionSpec as P

MESH = pl.DeviceIdType.MESH
ridge = 1.0
sentinel = 100.0
lanes = 128
slot = 8


def merge_pairs(lo, hi, r):
    step = r * 2
    if step < hi - lo:
        yield from merge_pairs(lo, hi, step)
        yield from merge_pairs(lo + r, hi, step)
        yield from ((i, i + r) for i in range(lo + r, hi - r, step))
    else:
        yield (lo, lo + r)


def sort_pairs(lo, hi):
    if hi - lo >= 1:
        mid = lo + (hi - lo) // 2
        yield from sort_pairs(lo, mid)
        yield from sort_pairs(mid + 1, hi)
        yield from merge_pairs(lo, hi, 1)


def sort_network(values):
    values = list(values)
    for i, j in sort_pairs(0, len(values) - 1):
        a, b = values[i], values[j]
        values[i], values[j] = jnp.minimum(a, b), jnp.maximum(a, b)
    return values


def kernel(
    n,
    pixes,
    x_ref,
    m_ref,
    days_ref,
    med_ref,
    slope_ref,
    wide,
    sent,
    got,
    part,
    parts,
    mean_row,
    mean_rows,
    mean_tile,
    year_tile,
    flip,
    data_send,
    data_recv,
    part_send,
    part_recv,
    mean_send,
    mean_recv,
    med_send,
    med_recv,
    slope_send,
    slope_recv,
):
    me = lax.axis_index("date")
    pix = lax.axis_index("pix")
    dates, bands, tile = x_ref.shape
    width = tile // n
    total = n * dates

    barrier = pltpu.get_barrier_semaphore()

    @pl.loop(1, n)
    def _(r):
        pl.semaphore_signal(barrier, inc=1, device_id={"date": lax.rem(me + r, n)}, device_id_type=MESH)

    for r in range(1, pixes):
        pl.semaphore_signal(barrier, inc=1, device_id={"pix": lax.rem(pix + r, pixes)}, device_id_type=MESH)

    def mark(j, carry):
        cols = pl.ds(pl.multiple_of(j * width, lanes), width)
        out = []
        for d in range(dates):
            x = x_ref[d, :, cols].astype(jnp.float32)
            valid = jnp.broadcast_to(m_ref[d : d + 1, cols], x.shape) > 0
            wide[d * bands : (d + 1) * bands, :] = jnp.where(valid, x, sentinel)
            csum, cnt = carry[d]
            csum = csum + jnp.where(valid, x, 0.0)
            cnt = cnt + jnp.where(valid, 1.0, 0.0)
            out.append((csum, cnt))
        sent[j] = wide[...].astype(jnp.bfloat16)
        return tuple(out)

    zero = jnp.zeros((bands, width), jnp.float32)
    sums = lax.fori_loop(0, n, mark, tuple((zero, zero) for _ in range(dates)))
    got[me] = sent[me]

    lane = lax.broadcasted_iota(jnp.int32, (bands, lanes), 1)
    band = lax.broadcasted_iota(jnp.int32, (bands, lanes), 0)
    lane_row = lax.broadcasted_iota(jnp.int32, (1, lanes), 1)
    row = jnp.zeros((bands, lanes), jnp.float32)
    count_row = jnp.zeros((bands, lanes), jnp.float32)
    for d in range(dates):
        csum = jnp.sum(sums[d][0], axis=1, keepdims=True)
        cnt = jnp.sum(sums[d][1], axis=1, keepdims=True)
        row = row + jnp.where(lane == d * slot + band, csum, 0.0)
        count_row = count_row + jnp.where((lane >= d * slot) & (lane < (d + 1) * slot) & (band == 0), cnt, 0.0)
    part[0:1, :] = jnp.sum(row, axis=0, keepdims=True)
    part[1:2, :] = jnp.sum(count_row, axis=0, keepdims=True)

    pl.semaphore_wait(barrier, n - 1 + pixes - 1)

    def part_copy(r):
        return pltpu.make_async_remote_copy(
            src_ref=part,
            dst_ref=parts.at[r],
            send_sem=part_send.at[r],
            recv_sem=part_recv.at[r],
            device_id={"pix": lax.rem(pix + r, pixes)},
            device_id_type=MESH,
        )

    for r in range(1, pixes):
        part_copy(r).start()

    def data_copy(r):
        j = lax.rem(me + r, n)
        return pltpu.make_async_remote_copy(
            src_ref=sent.at[j],
            dst_ref=got.at[me],
            send_sem=data_send.at[r],
            recv_sem=data_recv.at[r],
            device_id={"date": j},
            device_id_type=MESH,
        )

    @pl.loop(1, n)
    def _(r):
        data_copy(r).start()

    csum_row = part[0:1, :]
    cnt_row = part[1:2, :]
    for r in range(1, pixes):
        part_copy(r).wait_recv()
        csum_row = csum_row + parts[r, 0:1, :]
        cnt_row = cnt_row + parts[r, 1:2, :]
    means = csum_row / jnp.maximum(cnt_row, 1.0)
    for d in range(dates):
        year = jnp.full((1, lanes), days_ref[d], jnp.int32).astype(jnp.float32) / 365.0
        means = jnp.where(lane_row == d * slot + slot - 1, year, means)
    mean_row[...] = means
    mean_rows[me] = means

    def mean_copy(r):
        return pltpu.make_async_remote_copy(
            src_ref=mean_row,
            dst_ref=mean_rows.at[me],
            send_sem=mean_send.at[r],
            recv_sem=mean_recv.at[r],
            device_id={"date": lax.rem(me + r, n)},
            device_id_type=MESH,
        )

    @pl.loop(1, n)
    def _(r):
        mean_copy(r).start()

    @pl.loop(1, n)
    def _(r):
        mean_copy(r).wait_recv()

    @pl.loop(0, n)
    def _(j):
        line = jnp.broadcast_to(mean_rows[j], (bands, lanes))
        for d in range(dates):
            mean = jnp.sum(jnp.where(lane == d * slot + band, line, 0.0), axis=1, keepdims=True)
            year = jnp.sum(jnp.where(lane == d * slot + slot - 1, line, 0.0), axis=1, keepdims=True)
            mean_tile[j * dates + d] = jnp.broadcast_to(mean, (bands, lanes))
            year_tile[j * dates + d] = jnp.broadcast_to(year, (bands, lanes))

    @pl.loop(1, n)
    def _(r):
        data_copy(r).wait_recv()

    @pl.loop(0, width // lanes)
    def _(k):
        cols = pl.ds(pl.multiple_of(k * lanes, lanes), lanes)
        blank = jnp.zeros((bands, lanes), jnp.float32)

        def trend(j, carry):
            fill, s_zero, s_one, s_two, s_y, s_ty = carry
            block = got[j, :, cols].astype(jnp.float32)
            for d in range(dates):
                x = block[d * bands : (d + 1) * bands, :]
                year = year_tile[j * dates + d]
                valid = x < 50.0
                y = jnp.where(valid, x - mean_tile[j * dates + d], 0.0)
                m = jnp.where(valid, 1.0, 0.0)
                tm = year * m
                s_zero = s_zero + m
                s_one = s_one + tm
                s_two = s_two + year * tm
                s_y = s_y + y
                s_ty = s_ty + year * y
                flip[j * dates + d] = jnp.where(valid, x, fill)
                fill = jnp.where(valid, fill, -fill)
            return (fill, s_zero, s_one, s_two, s_y, s_ty)

        start = (blank + sentinel, blank, blank, blank, blank, blank)
        fill, s_zero, s_one, s_two, s_y, s_ty = lax.fori_loop(0, n, trend, start)
        first = s_zero + ridge
        slope = (first * s_ty - s_one * s_y) / (first * (s_two + ridge) - s_one * s_one)

        half = total // 2
        low = sort_network([flip[i] for i in range(half)])
        high = sort_network([flip[half + i] for i in range(half)])
        lower = None
        upper = None
        for i in range(half):
            a, b = low[i], high[half - 1 - i]
            small, large = jnp.minimum(a, b), jnp.maximum(a, b)
            lower = small if lower is None else jnp.maximum(lower, small)
            upper = large if upper is None else jnp.minimum(upper, large)
        median = jnp.where(fill < 0.0, lower, 0.5 * (lower + upper))
        here = pl.ds(pl.multiple_of(me * width + k * lanes, lanes), lanes)
        med_ref[:, here] = median
        slope_ref[:, here] = slope

    mine = pl.ds(pl.multiple_of(me * width, lanes), width)

    def out_copy(r, ref, send, recv):
        return pltpu.make_async_remote_copy(
            src_ref=ref.at[:, mine],
            dst_ref=ref.at[:, mine],
            send_sem=send.at[r],
            recv_sem=recv.at[r],
            device_id={"date": lax.rem(me + r, n)},
            device_id_type=MESH,
        )

    @pl.loop(1, n)
    def _(r):
        out_copy(r, med_ref, med_send, med_recv).start()
        out_copy(r, slope_ref, slope_send, slope_recv).start()

    for r in range(1, pixes):
        part_copy(r).wait_send()

    @pl.loop(1, n)
    def _(r):
        data_copy(r).wait_send()
        mean_copy(r).wait_send()

    @pl.loop(1, n)
    def _(r):
        out_copy(r, med_ref, med_send, med_recv).wait()
        out_copy(r, slope_ref, slope_send, slope_recv).wait()


def local(n, pixes, reflect, cloud_free, days):
    dates, bands, tile = reflect.shape
    width = tile // n
    out = jax.ShapeDtypeStruct((bands, tile), jnp.float32)
    vmem = pl.BlockSpec(memory_space=pltpu.VMEM)
    dma = pltpu.SemaphoreType.DMA
    return pl.pallas_call(
        functools.partial(kernel, n, pixes),
        out_shape=(out, out),
        in_specs=[vmem, vmem, pl.BlockSpec(memory_space=pltpu.SMEM)],
        out_specs=(vmem, vmem),
        scratch_shapes=[
            pltpu.VMEM((dates * bands, width), jnp.float32),
            pltpu.VMEM((n, dates * bands, width), jnp.bfloat16),
            pltpu.VMEM((n, dates * bands, width), jnp.bfloat16),
            pltpu.VMEM((2, lanes), jnp.float32),
            pltpu.VMEM((pixes, 2, lanes), jnp.float32),
            pltpu.VMEM((1, lanes), jnp.float32),
            pltpu.VMEM((n, 1, lanes), jnp.float32),
            pltpu.VMEM((n * dates, bands, lanes), jnp.float32),
            pltpu.VMEM((n * dates, bands, lanes), jnp.float32),
            pltpu.VMEM((n * dates, bands, lanes), jnp.float32),
            dma((n,)),
            dma((n,)),
            dma((pixes,)),
            dma((pixes,)),
            dma((n,)),
            dma((n,)),
            dma((n,)),
            dma((n,)),
            dma((n,)),
            dma((n,)),
        ],
        compiler_params=pltpu.CompilerParams(collective_id=0, has_side_effects=True),
    )(reflect, cloud_free, days)


def solution(mesh):
    placed = (P("date", None, "pix"), P("date", "pix"), P("date"))
    return jax.shard_map(
        functools.partial(local, mesh.shape["date"], mesh.shape["pix"]),
        mesh=mesh,
        in_specs=placed,
        out_specs=(P(None, "pix"), P(None, "pix")),
        check_vma=False,
    )
```

```python
import functools

import jax
import jax.numpy as jnp
from jax import lax
from jax.experimental import pallas as pl
from jax.experimental.pallas import tpu as pltpu
from jax.sharding import PartitionSpec as P

MESH = pl.DeviceIdType.MESH
ridge = 1.0
sentinel = 100.0
lanes = 128
slot = 8


def merge_pairs(lo, hi, r):
    step = r * 2
    if step < hi - lo:
        yield from merge_pairs(lo, hi, step)
        yield from merge_pairs(lo + r, hi, step)
        yield from ((i, i + r) for i in range(lo + r, hi - r, step))
    else:
        yield (lo, lo + r)


def sort_pairs(lo, hi):
    if hi - lo >= 1:
        mid = lo + (hi - lo) // 2
        yield from sort_pairs(lo, mid)
        yield from sort_pairs(mid + 1, hi)
        yield from merge_pairs(lo, hi, 1)


def sort_network(values):
    values = list(values)
    for i, j in sort_pairs(0, len(values) - 1):
        a, b = values[i], values[j]
        values[i], values[j] = jnp.minimum(a, b), jnp.maximum(a, b)
    return values


def kernel(
    n,
    pixes,
    group,
    x_hbm,
    m_hbm,
    days_ref,
    med_ref,
    slope_ref,
    x_ref,
    m_ref,
    wide,
    sent,
    got,
    part,
    parts,
    mean_row,
    mean_rows,
    stack,
    mean_tile,
    year_tile,
    flip,
    load_sem,
    data_send,
    data_recv,
    part_send,
    part_recv,
    mean_send,
    mean_recv,
    far_send,
    far_recv,
    near_send,
    near_recv,
):
    me = lax.axis_index("date")
    pix = lax.axis_index("pix")
    bands, dates, tile = x_ref.shape
    width = tile // n
    total = n * dates
    lines = n // group
    line = me // group
    spot = lax.rem(me, group)
    pieces = sent.shape[0]
    span = width // pieces

    barrier = pltpu.get_barrier_semaphore()

    @pl.loop(1, n)
    def _(r):
        pl.semaphore_signal(barrier, inc=1, device_id={"date": lax.rem(me + r, n)}, device_id_type=MESH)

    for r in range(1, pixes):
        pl.semaphore_signal(barrier, inc=1, device_id={"pix": lax.rem(pix + r, pixes)}, device_id_type=MESH)

    load_x = pltpu.make_async_copy(x_hbm, x_ref, load_sem.at[0])
    load_m = pltpu.make_async_copy(m_hbm, m_ref, load_sem.at[1])
    load_x.start()
    load_m.start()
    stack[...] = jnp.zeros_like(stack)
    load_m.wait()
    load_x.wait()

    def mark(j, carry):
        cols = pl.ds(pl.multiple_of(j * width, lanes), width)
        valid = m_ref[:, cols] > 0
        out = []
        for b in range(bands):
            x = x_ref[b, :, cols].astype(jnp.float32)
            marked = jnp.where(valid, x, sentinel)
            for d in range(dates):
                wide[d * bands + b : d * bands + b + 1, :] = marked[d : d + 1, :]
            out.append(carry[b] + jnp.where(valid, x, 0.0))
        for p in range(pieces):
            sent[p, j] = wide[:, p * span : (p + 1) * span].astype(jnp.bfloat16)
        out.append(carry[bands] + jnp.where(valid, 1.0, 0.0))
        return tuple(out)

    zero = jnp.zeros((dates, width), jnp.float32)
    sums = lax.fori_loop(0, n, mark, tuple(zero for _ in range(bands + 1)))
    for p in range(pieces):
        got[p, me] = sent[p, me]

    lane = lax.broadcasted_iota(jnp.int32, (dates, lanes), 1)
    date = lax.broadcasted_iota(jnp.int32, (dates, lanes), 0)
    lane_row = lax.broadcasted_iota(jnp.int32, (1, lanes), 1)
    row = jnp.zeros((dates, lanes), jnp.float32)
    for b in range(bands):
        row = row + jnp.where(lane == date * slot + b, jnp.sum(sums[b], axis=1, keepdims=True), 0.0)
    own = (lane >= date * slot) & (lane < (date + 1) * slot)
    count_row = jnp.where(own, jnp.sum(sums[bands], axis=1, keepdims=True), 0.0)
    part[0:1, :] = jnp.sum(row, axis=0, keepdims=True)
    part[1:2, :] = jnp.sum(count_row, axis=0, keepdims=True)

    pl.semaphore_wait(barrier, n - 1 + pixes - 1)

    def part_copy(r):
        return pltpu.make_async_remote_copy(
            src_ref=part,
            dst_ref=parts.at[r],
            send_sem=part_send.at[r],
            recv_sem=part_recv.at[r],
            device_id={"pix": lax.rem(pix + r, pixes)},
            device_id_type=MESH,
        )

    for r in range(1, pixes):
        part_copy(r).start()

    def data_copy(p, r):
        j = lax.rem(me + r, n)
        return pltpu.make_async_remote_copy(
            src_ref=sent.at[p, j],
            dst_ref=got.at[p, me],
            send_sem=data_send.at[p, r],
            recv_sem=data_recv.at[p, r],
            device_id={"date": j},
            device_id_type=MESH,
        )

    def mean_copy(r):
        return pltpu.make_async_remote_copy(
            src_ref=mean_row,
            dst_ref=mean_rows.at[me],
            send_sem=mean_send.at[r],
            recv_sem=mean_recv.at[r],
            device_id={"date": lax.rem(me + r, n)},
            device_id_type=MESH,
        )

    @pl.loop(1, n)
    def _(r):
        data_copy(0, r).start()

    csum_row = part[0:1, :]
    cnt_row = part[1:2, :]
    for r in range(1, pixes):
        part_copy(r).wait_recv()
        csum_row = csum_row + parts[r, 0:1, :]
        cnt_row = cnt_row + parts[r, 1:2, :]
    means = csum_row / jnp.maximum(cnt_row, 1.0)
    years = jnp.zeros((1, lanes), jnp.float32)
    for d in range(dates):
        year = jnp.full((1, lanes), days_ref[d], jnp.int32).astype(jnp.float32) / 365.0
        years = jnp.where((lane_row >= d * slot) & (lane_row < (d + 1) * slot), year, years)
    mean_row[0:1, :] = means
    mean_row[1:2, :] = years
    mean_rows[me] = mean_row[...]

    @pl.loop(1, n)
    def _(r):
        mean_copy(r).start()

    for p in range(1, pieces):

        @pl.loop(1, n)
        def _(r):
            data_copy(p, r).start()

    @pl.loop(1, n)
    def _(r):
        mean_copy(r).wait_recv()

    for row_index, out_ref in ((0, mean_tile), (1, year_tile)):
        for j in range(n):
            stack[j : j + 1, :] = mean_rows[j, row_index : row_index + 1, :]
        turned = jnp.transpose(stack[...])
        for j in range(n):
            for d in range(dates):
                column = turned[d * slot : d * slot + bands, j : j + 1]
                out_ref[j * dates + d] = jnp.broadcast_to(column, (bands, lanes))

    def rank(p, k):
        cols = pl.ds(pl.multiple_of(k * lanes, lanes), lanes)
        blank = jnp.zeros((bands, lanes), jnp.float32)

        def trend(j, carry):
            fill, s_zero, s_one, s_two, s_y, s_ty = carry
            block = got[p, j, :, cols].astype(jnp.float32)
            for d in range(dates):
                x = block[d * bands : (d + 1) * bands, :]
                year = year_tile[j * dates + d]
                valid = x < 50.0
                y = jnp.where(valid, x - mean_tile[j * dates + d], 0.0)
                m = jnp.where(valid, 1.0, 0.0)
                tm = year * m
                s_zero = s_zero + m
                s_one = s_one + tm
                s_two = s_two + year * tm
                s_y = s_y + y
                s_ty = s_ty + year * y
                flip[j * dates + d] = jnp.where(valid, x, fill)
                fill = jnp.where(valid, fill, -fill)
            return (fill, s_zero, s_one, s_two, s_y, s_ty)

        start = (blank + sentinel, blank, blank, blank, blank, blank)
        fill, s_zero, s_one, s_two, s_y, s_ty = lax.fori_loop(0, n, trend, start)
        first = s_zero + ridge
        slope = (first * s_ty - s_one * s_y) / (first * (s_two + ridge) - s_one * s_one)

        half = total // 2
        low = sort_network([flip[i] for i in range(half)])
        high = sort_network([flip[half + i] for i in range(half)])
        lower = None
        upper = None
        for i in range(half):
            a, b = low[i], high[half - 1 - i]
            small, large = jnp.minimum(a, b), jnp.maximum(a, b)
            lower = small if lower is None else jnp.maximum(lower, small)
            upper = large if upper is None else jnp.minimum(upper, large)
        median = jnp.where(fill < 0.0, lower, 0.5 * (lower + upper))
        here = pl.ds(pl.multiple_of(me * width + p * span + k * lanes, lanes), lanes)
        med_ref[:, here] = median
        slope_ref[:, here] = slope

    refs = (med_ref, slope_ref)

    def out_copy(ref, owner, p, target, send, recv):
        cols = pl.ds(pl.multiple_of(owner * width + p * span, lanes), span)
        return pltpu.make_async_remote_copy(
            src_ref=ref.at[:, cols],
            dst_ref=ref.at[:, cols],
            send_sem=send,
            recv_sem=recv,
            device_id={"date": target},
            device_id_type=MESH,
        )

    def far_copies(p, r):
        target = lax.rem(line + r, lines) * group + spot
        return [out_copy(refs[i], me, p, target, far_send.at[p, r, i], far_recv.at[p, r, i]) for i in range(2)]

    def near_copies(p, r, s):
        owner = lax.rem(line + lines - r, lines) * group + spot
        target = line * group + lax.rem(spot + s, group)
        return [
            out_copy(refs[i], owner, p, target, near_send.at[p, r, s, i], near_recv.at[p, r, s, i]) for i in range(2)
        ]

    for p in range(pieces):

        @pl.loop(1, n)
        def _(r):
            data_copy(p, r).wait_recv()

        @pl.loop(0, span // lanes)
        def _(k):
            rank(p, k)

        for r in range(1, lines):
            for copy in far_copies(p, r):
                copy.start()
        for s in range(1, group):
            for copy in near_copies(p, 0, s):
                copy.start()

    for p in range(pieces):
        for r in range(1, lines):
            for copy in far_copies(p, r):
                copy.wait_recv()
            for s in range(1, group):
                for copy in near_copies(p, r, s):
                    copy.start()

    for r in range(1, pixes):
        part_copy(r).wait_send()

    @pl.loop(1, n)
    def _(r):
        mean_copy(r).wait_send()
        for p in range(pieces):
            data_copy(p, r).wait_send()

    for p in range(pieces):
        for r in range(1, lines):
            for copy in far_copies(p, r):
                copy.wait_send()
        for r in range(lines):
            for s in range(1, group):
                for copy in near_copies(p, r, s):
                    copy.wait()


def local(n, pixes, reflect, cloud_free, days):
    dates, bands, tile = reflect.shape
    width = tile // n
    group = 1
    while group * group * 4 <= n and n % (group * 2) == 0:
        group *= 2
    pieces = 2 if width % (2 * lanes) == 0 else 1
    span = width // pieces
    lines = n // group
    turned = -(-n // lanes) * lanes
    out = jax.ShapeDtypeStruct((bands, tile), jnp.float32)
    vmem = pl.BlockSpec(memory_space=pltpu.VMEM)
    hbm = pl.BlockSpec(memory_space=pl.ANY)
    dma = pltpu.SemaphoreType.DMA
    return pl.pallas_call(
        functools.partial(kernel, n, pixes, group),
        out_shape=(out, out),
        in_specs=[hbm, hbm, pl.BlockSpec(memory_space=pltpu.SMEM)],
        out_specs=(vmem, vmem),
        scratch_shapes=[
            pltpu.VMEM((bands, dates, tile), jnp.bfloat16),
            pltpu.VMEM((dates, tile), jnp.int32),
            pltpu.VMEM((dates * bands, width), jnp.float32),
            pltpu.VMEM((pieces, n, dates * bands, span), jnp.bfloat16),
            pltpu.VMEM((pieces, n, dates * bands, span), jnp.bfloat16),
            pltpu.VMEM((2, lanes), jnp.float32),
            pltpu.VMEM((pixes, 2, lanes), jnp.float32),
            pltpu.VMEM((2, lanes), jnp.float32),
            pltpu.VMEM((n, 2, lanes), jnp.float32),
            pltpu.VMEM((turned, lanes), jnp.float32),
            pltpu.VMEM((n * dates, bands, lanes), jnp.float32),
            pltpu.VMEM((n * dates, bands, lanes), jnp.float32),
            pltpu.VMEM((n * dates, bands, lanes), jnp.float32),
            dma((2,)),
            dma((pieces, n)),
            dma((pieces, n)),
            dma((pixes,)),
            dma((pixes,)),
            dma((n,)),
            dma((n,)),
            dma((pieces, lines, 2)),
            dma((pieces, lines, 2)),
            dma((pieces, lines, group, 2)),
            dma((pieces, lines, group, 2)),
        ],
        compiler_params=pltpu.CompilerParams(collective_id=0, has_side_effects=True),
    )(jnp.transpose(reflect, (1, 0, 2)), cloud_free, days)


def solution(mesh):
    placed = (P("date", None, "pix"), P("date", "pix"), P("date"))
    return jax.shard_map(
        functools.partial(local, mesh.shape["date"], mesh.shape["pix"]),
        mesh=mesh,
        in_specs=placed,
        out_specs=(P(None, "pix"), P(None, "pix")),
        check_vma=False,
    )
```

```python
import functools

import jax
import jax.numpy as jnp
from jax import lax
from jax.experimental import pallas as pl
from jax.experimental.pallas import tpu as pltpu
from jax.sharding import PartitionSpec as P

MESH = pl.DeviceIdType.MESH
ridge = 1.0
sentinel = 100.0
lanes = 128
slot = 8


def merge_pairs(lo, hi, r):
    step = r * 2
    if step < hi - lo:
        yield from merge_pairs(lo, hi, step)
        yield from merge_pairs(lo + r, hi, step)
        yield from ((i, i + r) for i in range(lo + r, hi - r, step))
    else:
        yield (lo, lo + r)


def sort_pairs(lo, hi):
    if hi - lo >= 1:
        mid = lo + (hi - lo) // 2
        yield from sort_pairs(lo, mid)
        yield from sort_pairs(mid + 1, hi)
        yield from merge_pairs(lo, hi, 1)


def sort_network(values):
    values = list(values)
    for i, j in sort_pairs(0, len(values) - 1):
        a, b = values[i], values[j]
        values[i], values[j] = jnp.minimum(a, b), jnp.maximum(a, b)
    return values


def kernel(
    n,
    pixes,
    group,
    x_hbm,
    m_hbm,
    days_ref,
    out_ref,
    x_ref,
    m_ref,
    wide,
    sent,
    got,
    part,
    parts,
    mean_row,
    mean_rows,
    stack,
    mean_tile,
    year_tile,
    flip,
    load_sem,
    data_send,
    data_recv,
    part_send,
    part_recv,
    mean_send,
    mean_recv,
    far_send,
    far_recv,
    near_send,
    near_recv,
):
    me = lax.axis_index("date")
    pix = lax.axis_index("pix")
    bands, dates, tile = x_ref.shape
    width = tile // n
    total = n * dates
    lines = n // group
    line = me // group
    spot = lax.rem(me, group)
    pieces = sent.shape[0]
    span = width // pieces

    barrier = pltpu.get_barrier_semaphore()

    @pl.loop(1, n)
    def _(r):
        pl.semaphore_signal(barrier, inc=1, device_id={"date": lax.rem(me + r, n)}, device_id_type=MESH)

    for r in range(1, pixes):
        pl.semaphore_signal(barrier, inc=1, device_id={"pix": lax.rem(pix + r, pixes)}, device_id_type=MESH)

    load_x = pltpu.make_async_copy(x_hbm, x_ref, load_sem.at[0])
    load_m = pltpu.make_async_copy(m_hbm, m_ref, load_sem.at[1])
    load_x.start()
    load_m.start()
    stack[...] = jnp.zeros_like(stack)
    load_m.wait()
    load_x.wait()

    def mark(j, carry):
        cols = pl.ds(pl.multiple_of(j * width, lanes), width)
        valid = m_ref[:, cols] > 0
        out = []
        for b in range(bands):
            x = x_ref[b, :, cols].astype(jnp.float32)
            marked = jnp.where(valid, x, sentinel)
            for d in range(dates):
                wide[d * bands + b : d * bands + b + 1, :] = marked[d : d + 1, :]
            out.append(carry[b] + jnp.where(valid, x, 0.0))
        for p in range(pieces):
            sent[p, j] = wide[:, p * span : (p + 1) * span].astype(jnp.bfloat16)
        out.append(carry[bands] + jnp.where(valid, 1.0, 0.0))
        return tuple(out)

    zero = jnp.zeros((dates, width), jnp.float32)
    sums = lax.fori_loop(0, n, mark, tuple(zero for _ in range(bands + 1)))
    for p in range(pieces):
        got[p, me] = sent[p, me]

    lane = lax.broadcasted_iota(jnp.int32, (dates, lanes), 1)
    date = lax.broadcasted_iota(jnp.int32, (dates, lanes), 0)
    lane_row = lax.broadcasted_iota(jnp.int32, (1, lanes), 1)
    row = jnp.zeros((dates, lanes), jnp.float32)
    for b in range(bands):
        row = row + jnp.where(lane == date * slot + b, jnp.sum(sums[b], axis=1, keepdims=True), 0.0)
    own = (lane >= date * slot) & (lane < (date + 1) * slot)
    count_row = jnp.where(own, jnp.sum(sums[bands], axis=1, keepdims=True), 0.0)
    part[0:1, :] = jnp.sum(row, axis=0, keepdims=True)
    part[1:2, :] = jnp.sum(count_row, axis=0, keepdims=True)

    pl.semaphore_wait(barrier, n - 1 + pixes - 1)

    def part_copy(r):
        return pltpu.make_async_remote_copy(
            src_ref=part,
            dst_ref=parts.at[r],
            send_sem=part_send.at[r],
            recv_sem=part_recv.at[r],
            device_id={"pix": lax.rem(pix + r, pixes)},
            device_id_type=MESH,
        )

    for r in range(1, pixes):
        part_copy(r).start()

    def data_copy(p, r):
        j = lax.rem(me + r, n)
        return pltpu.make_async_remote_copy(
            src_ref=sent.at[p, j],
            dst_ref=got.at[p, me],
            send_sem=data_send.at[p, r],
            recv_sem=data_recv.at[p, r],
            device_id={"date": j},
            device_id_type=MESH,
        )

    def mean_copy(r):
        return pltpu.make_async_remote_copy(
            src_ref=mean_row,
            dst_ref=mean_rows.at[me],
            send_sem=mean_send.at[r],
            recv_sem=mean_recv.at[r],
            device_id={"date": lax.rem(me + r, n)},
            device_id_type=MESH,
        )

    @pl.loop(1, n)
    def _(r):
        data_copy(0, r).start()

    csum_row = part[0:1, :]
    cnt_row = part[1:2, :]
    for r in range(1, pixes):
        part_copy(r).wait_recv()
        csum_row = csum_row + parts[r, 0:1, :]
        cnt_row = cnt_row + parts[r, 1:2, :]
    means = csum_row / jnp.maximum(cnt_row, 1.0)
    years = jnp.zeros((1, lanes), jnp.float32)
    for d in range(dates):
        year = jnp.full((1, lanes), days_ref[d], jnp.int32).astype(jnp.float32) / 365.0
        years = jnp.where((lane_row >= d * slot) & (lane_row < (d + 1) * slot), year, years)
    mean_row[0:1, :] = means
    mean_row[1:2, :] = years
    mean_rows[me] = mean_row[...]

    @pl.loop(1, n)
    def _(r):
        mean_copy(r).start()

    for p in range(1, pieces):

        @pl.loop(1, n)
        def _(r):
            data_copy(p, r).start()

    @pl.loop(1, n)
    def _(r):
        mean_copy(r).wait_recv()

    for row_index, tile_ref in ((0, mean_tile), (1, year_tile)):
        for j in range(n):
            stack[j : j + 1, :] = mean_rows[j, row_index : row_index + 1, :]
        turned = jnp.transpose(stack[...])
        for j in range(n):
            for d in range(dates):
                column = turned[d * slot : d * slot + bands, j : j + 1]
                tile_ref[j * dates + d] = jnp.broadcast_to(column, (bands, lanes))

    def rank(p, k):
        cols = pl.ds(pl.multiple_of(k * lanes, lanes), lanes)
        blank = jnp.zeros((bands, lanes), jnp.float32)

        def trend(j, carry):
            fill, s_zero, s_one, s_two, s_y, s_ty = carry
            block = got[p, j, :, cols].astype(jnp.float32)
            for d in range(dates):
                x = block[d * bands : (d + 1) * bands, :]
                year = year_tile[j * dates + d]
                valid = x < 50.0
                y = jnp.where(valid, x - mean_tile[j * dates + d], 0.0)
                m = jnp.where(valid, 1.0, 0.0)
                tm = year * m
                s_zero = s_zero + m
                s_one = s_one + tm
                s_two = s_two + year * tm
                s_y = s_y + y
                s_ty = s_ty + year * y
                flip[j * dates + d] = jnp.where(valid, x, fill)
                fill = jnp.where(valid, fill, -fill)
            return (fill, s_zero, s_one, s_two, s_y, s_ty)

        start = (blank + sentinel, blank, blank, blank, blank, blank)
        fill, s_zero, s_one, s_two, s_y, s_ty = lax.fori_loop(0, n, trend, start)
        first = s_zero + ridge
        slope = (first * s_ty - s_one * s_y) / (first * (s_two + ridge) - s_one * s_one)

        half = total // 2
        low = sort_network([flip[i] for i in range(half)])
        high = sort_network([flip[half + i] for i in range(half)])
        lower = None
        upper = None
        for i in range(half):
            a, b = low[i], high[half - 1 - i]
            small, large = jnp.minimum(a, b), jnp.maximum(a, b)
            lower = small if lower is None else jnp.maximum(lower, small)
            upper = large if upper is None else jnp.minimum(upper, large)
        median = jnp.where(fill < 0.0, lower, 0.5 * (lower + upper))
        here = pl.ds(pl.multiple_of(me * width + p * span + k * lanes, lanes), lanes)
        out_ref[0, :, here] = median
        out_ref[1, :, here] = slope

    def out_copy(owner, p, target, send, recv):
        cols = pl.ds(pl.multiple_of(owner * width + p * span, lanes), span)
        return pltpu.make_async_remote_copy(
            src_ref=out_ref.at[:, :, cols],
            dst_ref=out_ref.at[:, :, cols],
            send_sem=send,
            recv_sem=recv,
            device_id={"date": target},
            device_id_type=MESH,
        )

    def far_copy(p, r):
        target = lax.rem(line + r, lines) * group + spot
        return out_copy(me, p, target, far_send.at[p, r], far_recv.at[p, r])

    def near_copy(p, r, s):
        owner = lax.rem(line + lines - r, lines) * group + spot
        target = line * group + lax.rem(spot + s, group)
        return out_copy(owner, p, target, near_send.at[p, r, s], near_recv.at[p, r, s])

    for p in range(pieces):

        @pl.loop(1, n)
        def _(r):
            data_copy(p, r).wait_recv()

        @pl.loop(0, span // lanes)
        def _(k):
            rank(p, k)

        for r in range(1, lines):
            far_copy(p, r).start()
        for s in range(1, group):
            near_copy(p, 0, s).start()

    for p in range(pieces):
        for r in range(1, lines):
            far_copy(p, r).wait_recv()
            for s in range(1, group):
                near_copy(p, r, s).start()

    for r in range(1, pixes):
        part_copy(r).wait_send()

    @pl.loop(1, n)
    def _(r):
        mean_copy(r).wait_send()
        for p in range(pieces):
            data_copy(p, r).wait_send()

    for p in range(pieces):
        for r in range(1, lines):
            far_copy(p, r).wait_send()
        for r in range(lines):
            for s in range(1, group):
                near_copy(p, r, s).wait()


def local(n, pixes, reflect, cloud_free, days):
    dates, bands, tile = reflect.shape
    width = tile // n
    group = 1
    while group * group * 4 <= n and n % (group * 2) == 0:
        group *= 2
    pieces = 2 if width % (2 * lanes) == 0 else 1
    span = width // pieces
    lines = n // group
    turned = -(-n // lanes) * lanes
    vmem = pl.BlockSpec(memory_space=pltpu.VMEM)
    hbm = pl.BlockSpec(memory_space=pl.ANY)
    dma = pltpu.SemaphoreType.DMA
    out = pl.pallas_call(
        functools.partial(kernel, n, pixes, group),
        out_shape=pltpu.VMEM((2, bands, tile), jnp.float32),
        in_specs=[hbm, hbm, pl.BlockSpec(memory_space=pltpu.SMEM)],
        out_specs=vmem,
        scratch_shapes=[
            pltpu.VMEM((bands, dates, tile), jnp.bfloat16),
            pltpu.VMEM((dates, tile), jnp.int32),
            pltpu.VMEM((dates * bands, width), jnp.float32),
            pltpu.VMEM((pieces, n, dates * bands, span), jnp.bfloat16),
            pltpu.VMEM((pieces, n, dates * bands, span), jnp.bfloat16),
            pltpu.VMEM((2, lanes), jnp.float32),
            pltpu.VMEM((pixes, 2, lanes), jnp.float32),
            pltpu.VMEM((2, lanes), jnp.float32),
            pltpu.VMEM((n, 2, lanes), jnp.float32),
            pltpu.VMEM((turned, lanes), jnp.float32),
            pltpu.VMEM((n * dates, bands, lanes), jnp.float32),
            pltpu.VMEM((n * dates, bands, lanes), jnp.float32),
            pltpu.VMEM((n * dates, bands, lanes), jnp.float32),
            dma((2,)),
            dma((pieces, n)),
            dma((pieces, n)),
            dma((pixes,)),
            dma((pixes,)),
            dma((n,)),
            dma((n,)),
            dma((pieces, lines)),
            dma((pieces, lines)),
            dma((pieces, lines, group)),
            dma((pieces, lines, group)),
        ],
        compiler_params=pltpu.CompilerParams(collective_id=0, has_side_effects=True),
    )(jnp.transpose(reflect, (1, 0, 2)), cloud_free, days)
    return (out[0], out[1])


def solution(mesh):
    placed = (P("date", None, "pix"), P("date", "pix"), P("date"))
    return jax.shard_map(
        functools.partial(local, mesh.shape["date"], mesh.shape["pix"]),
        mesh=mesh,
        in_specs=placed,
        out_specs=(P(None, "pix"), P(None, "pix")),
        check_vma=False,
    )
```

```python
import functools

import jax
import jax.numpy as jnp
from jax import lax
from jax.experimental import pallas as pl
from jax.experimental.pallas import tpu as pltpu
from jax.sharding import PartitionSpec as P

MESH = pl.DeviceIdType.MESH
ridge = 1.0
sentinel = 100.0
lanes = 128
slot = 8


def merge_pairs(lo, hi, r):
    step = r * 2
    if step < hi - lo:
        yield from merge_pairs(lo, hi, step)
        yield from merge_pairs(lo + r, hi, step)
        yield from ((i, i + r) for i in range(lo + r, hi - r, step))
    else:
        yield (lo, lo + r)


def sort_pairs(lo, hi):
    if hi - lo >= 1:
        mid = lo + (hi - lo) // 2
        yield from sort_pairs(lo, mid)
        yield from sort_pairs(mid + 1, hi)
        yield from merge_pairs(lo, hi, 1)


def sort_network(values):
    values = list(values)
    for i, j in sort_pairs(0, len(values) - 1):
        a, b = values[i], values[j]
        values[i], values[j] = jnp.minimum(a, b), jnp.maximum(a, b)
    return values


def kernel(
    n,
    pixes,
    group,
    x_hbm,
    m_hbm,
    days_ref,
    out_ref,
    x_ref,
    m_ref,
    wide,
    sent,
    got,
    part,
    parts,
    mean_row,
    mean_rows,
    stack,
    mean_tile,
    year_tile,
    flip,
    odd,
    load_sem,
    data_send,
    data_recv,
    part_send,
    part_recv,
    mean_send,
    mean_recv,
    far_send,
    far_recv,
    near_send,
    near_recv,
):
    me = lax.axis_index("date")
    pix = lax.axis_index("pix")
    bands, dates, tile = x_ref.shape
    width = tile // n
    total = n * dates
    lines = n // group
    line = me // group
    spot = lax.rem(me, group)
    pieces = sent.shape[0]
    span = width // pieces

    barrier = pltpu.get_barrier_semaphore()

    @pl.loop(1, n)
    def _(r):
        pl.semaphore_signal(barrier, inc=1, device_id={"date": lax.rem(me + r, n)}, device_id_type=MESH)

    for r in range(1, pixes):
        pl.semaphore_signal(barrier, inc=1, device_id={"pix": lax.rem(pix + r, pixes)}, device_id_type=MESH)

    load_x = pltpu.make_async_copy(x_hbm, x_ref, load_sem.at[0])
    load_m = pltpu.make_async_copy(m_hbm, m_ref, load_sem.at[1])
    load_x.start()
    load_m.start()
    stack[...] = jnp.zeros_like(stack)
    load_m.wait()
    load_x.wait()

    def mark(j, carry):
        cols = pl.ds(pl.multiple_of(j * width, lanes), width)
        valid = m_ref[:, cols] > 0
        out = []
        for b in range(bands):
            x = x_ref[b, :, cols].astype(jnp.float32)
            marked = jnp.where(valid, x, sentinel)
            for d in range(dates):
                wide[d * bands + b : d * bands + b + 1, :] = marked[d : d + 1, :]
            out.append(carry[b] + jnp.where(valid, x, 0.0))
        for p in range(pieces):
            sent[p, j] = wide[:, p * span : (p + 1) * span].astype(jnp.bfloat16)
        out.append(carry[bands] + jnp.where(valid, 1.0, 0.0))
        return tuple(out)

    zero = jnp.zeros((dates, width), jnp.float32)
    sums = lax.fori_loop(0, n, mark, tuple(zero for _ in range(bands + 1)))
    for p in range(pieces):
        got[p, me] = sent[p, me]

    lane = lax.broadcasted_iota(jnp.int32, (dates, lanes), 1)
    date = lax.broadcasted_iota(jnp.int32, (dates, lanes), 0)
    lane_row = lax.broadcasted_iota(jnp.int32, (1, lanes), 1)
    row = jnp.zeros((dates, lanes), jnp.float32)
    for b in range(bands):
        row = row + jnp.where(lane == date * slot + b, jnp.sum(sums[b], axis=1, keepdims=True), 0.0)
    own = (lane >= date * slot) & (lane < (date + 1) * slot)
    count_row = jnp.where(own, jnp.sum(sums[bands], axis=1, keepdims=True), 0.0)
    part[0:1, :] = jnp.sum(row, axis=0, keepdims=True)
    part[1:2, :] = jnp.sum(count_row, axis=0, keepdims=True)

    pl.semaphore_wait(barrier, n - 1 + pixes - 1)

    def part_copy(r):
        return pltpu.make_async_remote_copy(
            src_ref=part,
            dst_ref=parts.at[r],
            send_sem=part_send.at[r],
            recv_sem=part_recv.at[r],
            device_id={"pix": lax.rem(pix + r, pixes)},
            device_id_type=MESH,
        )

    for r in range(1, pixes):
        part_copy(r).start()

    def data_copy(p, r):
        j = lax.rem(me + r, n)
        return pltpu.make_async_remote_copy(
            src_ref=sent.at[p, j],
            dst_ref=got.at[p, me],
            send_sem=data_send.at[p, r],
            recv_sem=data_recv.at[p, r],
            device_id={"date": j},
            device_id_type=MESH,
        )

    def mean_copy(r):
        return pltpu.make_async_remote_copy(
            src_ref=mean_row,
            dst_ref=mean_rows.at[me],
            send_sem=mean_send.at[r],
            recv_sem=mean_recv.at[r],
            device_id={"date": lax.rem(me + r, n)},
            device_id_type=MESH,
        )

    @pl.loop(1, n)
    def _(r):
        data_copy(0, r).start()

    csum_row = part[0:1, :]
    cnt_row = part[1:2, :]
    for r in range(1, pixes):
        part_copy(r).wait_recv()
        csum_row = csum_row + parts[r, 0:1, :]
        cnt_row = cnt_row + parts[r, 1:2, :]
    means = csum_row / jnp.maximum(cnt_row, 1.0)
    years = jnp.zeros((1, lanes), jnp.float32)
    for d in range(dates):
        year = jnp.full((1, lanes), days_ref[d], jnp.int32).astype(jnp.float32) / 365.0
        years = jnp.where((lane_row >= d * slot) & (lane_row < (d + 1) * slot), year, years)
    mean_row[0:1, :] = means
    mean_row[1:2, :] = years
    mean_rows[me] = mean_row[...]

    @pl.loop(1, n)
    def _(r):
        mean_copy(r).start()

    for p in range(1, pieces):

        @pl.loop(1, n)
        def _(r):
            data_copy(p, r).start()

    @pl.loop(1, n)
    def _(r):
        mean_copy(r).wait_recv()

    for row_index, tile_ref in ((0, mean_tile), (1, year_tile)):
        for j in range(n):
            stack[j : j + 1, :] = mean_rows[j, row_index : row_index + 1, :]
        turned = jnp.transpose(stack[...])
        for j in range(n):
            for d in range(dates):
                column = turned[d * slot : d * slot + bands, j : j + 1]
                tile_ref[j * dates + d] = jnp.broadcast_to(column, (bands, lanes))

    def trend(p, r, carry):
        j = lax.rem(me + n - r, n)
        fill, s_zero, s_one, s_two, s_y, s_ty = carry
        block = got[p, j].astype(jnp.float32)
        for d in range(dates):
            x = block[d * bands : (d + 1) * bands, :]
            year = jnp.concatenate([year_tile[j * dates + d]] * (span // lanes), axis=1)
            mean = jnp.concatenate([mean_tile[j * dates + d]] * (span // lanes), axis=1)
            valid = x < 50.0
            y = jnp.where(valid, x - mean, 0.0)
            m = jnp.where(valid, 1.0, 0.0)
            tm = year * m
            s_zero = s_zero + m
            s_one = s_one + tm
            s_two = s_two + year * tm
            s_y = s_y + y
            s_ty = s_ty + year * y
            flip[r * dates + d] = jnp.where(valid, x, fill)
            fill = jnp.where(valid, fill, -fill)
        return (fill, s_zero, s_one, s_two, s_y, s_ty)

    def rank(p):
        blank = jnp.zeros((bands, span), jnp.float32)
        start = trend(p, 0, (blank + sentinel, blank, blank, blank, blank, blank))

        def arrived(r, carry):
            data_copy(p, r).wait_recv()
            return trend(p, r, carry)

        fill, s_zero, s_one, s_two, s_y, s_ty = lax.fori_loop(1, n, arrived, start)
        first = s_zero + ridge
        here = pl.ds(pl.multiple_of(me * width + p * span, lanes), span)
        out_ref[1, :, here] = (first * s_ty - s_one * s_y) / (first * (s_two + ridge) - s_one * s_one)
        odd[...] = jnp.where(fill < 0.0, 1.0, 0.0)

        @pl.loop(0, span // lanes)
        def _(k):
            cols = pl.ds(pl.multiple_of(k * lanes, lanes), lanes)
            half = total // 2
            low = sort_network([flip[i, :, cols] for i in range(half)])
            high = sort_network([flip[half + i, :, cols] for i in range(half)])
            lower = None
            upper = None
            for i in range(half):
                a, b = low[i], high[half - 1 - i]
                small, large = jnp.minimum(a, b), jnp.maximum(a, b)
                lower = small if lower is None else jnp.maximum(lower, small)
                upper = large if upper is None else jnp.minimum(upper, large)
            median = jnp.where(odd[:, cols] > 0.5, lower, 0.5 * (lower + upper))
            there = pl.ds(pl.multiple_of(me * width + p * span + k * lanes, lanes), lanes)
            out_ref[0, :, there] = median

    def out_copy(owner, p, target, send, recv):
        cols = pl.ds(pl.multiple_of(owner * width + p * span, lanes), span)
        return pltpu.make_async_remote_copy(
            src_ref=out_ref.at[:, :, cols],
            dst_ref=out_ref.at[:, :, cols],
            send_sem=send,
            recv_sem=recv,
            device_id={"date": target},
            device_id_type=MESH,
        )

    def partner(r):
        other = line
        for bit in range(lines.bit_length() - 1):
            if (r >> bit) & 1:
                other = other + (1 << bit) - (1 << (bit + 1)) * lax.rem(line // (1 << bit), 2)
        return other

    def far_copy(p, r):
        target = partner(r) * group + spot
        return out_copy(me, p, target, far_send.at[p, r], far_recv.at[p, r])

    def near_copy(p, r, s):
        owner = partner(r) * group + spot
        target = line * group + lax.rem(spot + s, group)
        return out_copy(owner, p, target, near_send.at[p, r, s], near_recv.at[p, r, s])

    for p in range(pieces):
        rank(p)

        for r in range(lines - 1, 0, -1):
            far_copy(p, r).start()
        for s in range(1, group):
            near_copy(p, 0, s).start()

    for p in range(pieces):
        for r in range(1, lines):
            far_copy(p, r).wait_recv()
            for s in range(1, group):
                near_copy(p, r, s).start()

    for r in range(1, pixes):
        part_copy(r).wait_send()

    @pl.loop(1, n)
    def _(r):
        mean_copy(r).wait_send()
        for p in range(pieces):
            data_copy(p, r).wait_send()

    for p in range(pieces):
        for r in range(1, lines):
            far_copy(p, r).wait_send()
        for r in range(lines):
            for s in range(1, group):
                near_copy(p, r, s).wait()


def local(n, pixes, reflect, cloud_free, days):
    dates, bands, tile = reflect.shape
    width = tile // n
    group = 1
    while group * group * 4 <= n and n % (group * 2) == 0:
        group *= 2
    pieces = 2 if width % (2 * lanes) == 0 else 1
    span = width // pieces
    lines = n // group
    turned = -(-n // lanes) * lanes
    vmem = pl.BlockSpec(memory_space=pltpu.VMEM)
    hbm = pl.BlockSpec(memory_space=pl.ANY)
    dma = pltpu.SemaphoreType.DMA
    out = pl.pallas_call(
        functools.partial(kernel, n, pixes, group),
        out_shape=pltpu.VMEM((2, bands, tile), jnp.float32),
        in_specs=[hbm, hbm, pl.BlockSpec(memory_space=pltpu.SMEM)],
        out_specs=vmem,
        scratch_shapes=[
            pltpu.VMEM((bands, dates, tile), jnp.bfloat16),
            pltpu.VMEM((dates, tile), jnp.int32),
            pltpu.VMEM((dates * bands, width), jnp.float32),
            pltpu.VMEM((pieces, n, dates * bands, span), jnp.bfloat16),
            pltpu.VMEM((pieces, n, dates * bands, span), jnp.bfloat16),
            pltpu.VMEM((2, lanes), jnp.float32),
            pltpu.VMEM((pixes, 2, lanes), jnp.float32),
            pltpu.VMEM((2, lanes), jnp.float32),
            pltpu.VMEM((n, 2, lanes), jnp.float32),
            pltpu.VMEM((turned, lanes), jnp.float32),
            pltpu.VMEM((n * dates, bands, lanes), jnp.float32),
            pltpu.VMEM((n * dates, bands, lanes), jnp.float32),
            pltpu.VMEM((n * dates, bands, span), jnp.float32),
            pltpu.VMEM((bands, span), jnp.float32),
            dma((2,)),
            dma((pieces, n)),
            dma((pieces, n)),
            dma((pixes,)),
            dma((pixes,)),
            dma((n,)),
            dma((n,)),
            dma((pieces, lines)),
            dma((pieces, lines)),
            dma((pieces, lines, group)),
            dma((pieces, lines, group)),
        ],
        compiler_params=pltpu.CompilerParams(collective_id=0, has_side_effects=True),
    )(jnp.transpose(reflect, (1, 0, 2)), cloud_free, days)
    return (out[0], out[1])


def solution(mesh):
    placed = (P("date", None, "pix"), P("date", "pix"), P("date"))
    return jax.shard_map(
        functools.partial(local, mesh.shape["date"], mesh.shape["pix"]),
        mesh=mesh,
        in_specs=placed,
        out_specs=(P(None, "pix"), P(None, "pix")),
        check_vma=False,
    )
```
